32 devices in a mesh: patch: 8 (over z, x), member: 4 (over y, core).
Axes of the slice: x: 2, y: 2, z: 4, core: 2. Of those that a mesh axis runs over, the one named last changes fastest.
Arguments:
- background: bfloat16 [32, 16, 3, 64, 128], P('patch', None, None, 'member'), may hold values from -6 to 6
- patch_blocks: int32 [32], replicated, may hold values from 1 to 16, as said below
- obs_values: float32 [16384], P(('patch', 'member')), may hold values from -12 to 12
- obs_errors: float32 [16384], P(('patch', 'member')), may hold values from 0.5 to 2
- obs_patch: int32 [16384], P('patch'), may hold values from 0 to 3
- obs_position: int32 [16384], P('patch'), may hold values from 0 to 1073741823
Outputs:
- analysis: bfloat16 [32, 16, 3, 64, 128], P('patch', None, None, 'member')
- inflation: float32 [], replicated
The draws below stay inside these ranges and needn't reach their ends.
Inputs may be any that keep to these rules, and one draw needn't show every extreme that they name: `obs_patch`: index among the 4 patches held by the observation's index of patch. `patch_blocks`: the used blocks of the 4 patches of one index of patch sum to at most 32; some index reaches 32, and some patch uses all 16.
All inputs are finite; a program needn't handle non-finite values.
Results may differ from the reference program's by a relative error of at most 0.0065.
Values may be sent and summed in bfloat16 or wider, within the bound.
A program may use at most 64 MiB of HBM per device.

```python
import math
import jax
import jax.numpy as jnp
from jax import lax

K = 64
NV = 3
CB = 128
MAXB = 16
DEV_BLOCKS = 32
NS_STEPS = 4
PD = 4
OBS_DEV = 2048
NP = 32
NOBS = 16384
N_PATCH = 8


def draw_patch_blocks(key, part):
    group_count = NP // PD
    extra_per = MAXB - 1
    position_count = PD * extra_per
    totals = jax.random.randint(jax.random.fold_in(key, 11), (group_count,), PD, DEV_BLOCKS + 1)
    mandatory_pick = jax.random.randint(jax.random.fold_in(key, 12), (), 0, group_count)
    favoured_position = jax.random.randint(jax.random.fold_in(key, 14), (), 0, PD)
    tile_clusters = jnp.arange(group_count, dtype=jnp.int32)
    totals = jnp.where(tile_clusters == mandatory_pick, DEV_BLOCKS, totals)
    order_keys = jax.random.split(jax.random.fold_in(key, 13), group_count)

    def shuffle(order_key):
        return jax.random.permutation(order_key, position_count).astype(jnp.int32)
    position_orderings = jax.vmap(shuffle)(order_keys)
    tile_at_position = jnp.arange(position_count, dtype=jnp.int32) // extra_per
    urgency_reward = jnp.where((tile_clusters == mandatory_pick)[:, None] & (tile_at_position != favoured_position)[None, :], position_count, 0)
    siting_merit = position_orderings + urgency_reward
    position = jnp.argsort(jnp.argsort(siting_merit, axis=1, stable=True), axis=1, stable=True)
    taken = position < (totals - PD)[:, None]
    patch_table = jnp.arange(PD, dtype=jnp.int32)
    belongs = tile_at_position[None, :, None] == patch_table[None, None, :]
    counts = jnp.sum(jnp.where(taken[:, :, None] & belongs, 1, 0), axis=1)
    return (counts + 1).reshape(group_count * PD).astype(jnp.int32)


def plant(values, own_key, least, top_value):
    index_at = [jax.random.randint(jax.random.fold_in(own_key, axis), (), 0, length) for axis, length in enumerate(values.shape)]
    widest = values.shape.index(max(values.shape))
    next_to = index_at[:widest] + [(index_at[widest] + 1) % values.shape[widest]] + index_at[widest + 1:]
    return values.at[tuple(index_at)].set(least).at[tuple(next_to)].set(top_value)


def block_scale(own_key, extent, cuts, least, largest):
    def one(dim, blocks):
        heights = jax.random.uniform(jax.random.fold_in(jax.random.fold_in(own_key, 6), dim), (blocks,), jnp.float32, least / len(cuts), largest / len(cuts))
        return jnp.repeat(jnp.exp(heights), extent[dim] // blocks).reshape((-1,) + (1,) * (len(extent) - dim - 1))

    loudness = one(*cuts[0])
    for cut in cuts[1:]:
        loudness = loudness * one(*cut)
    return loudness


def noise(stream_key, extent, scale, most, cuts=(), held_as=jnp.bfloat16):
    drawn = jax.random.normal(stream_key, extent, jnp.float32) * scale
    if len(cuts) > 0:
        drawn = block_scale(stream_key, extent, cuts, -0.22, 0.18) * drawn
    return jnp.clip(drawn, min=-most, max=most).astype(held_as)


def setup_inputs(seed: int = 0) -> dict:
    streams_of = jax.random.split(jax.random.key(seed), 7)
    background = noise(streams_of[0], (NP, MAXB, NV, K, CB), 1.0, 6.0, ((0, 8), (3, 4)))
    patch_blocks = draw_patch_blocks(jax.random.fold_in(streams_of[6], 71), 0)
    obs_values = noise(streams_of[2], (NOBS,), 2.0, 12.0, ((0, 32),), jnp.float32)
    obs_errors = jnp.clip(jnp.exp(math.log(2.0) - 1.3862944 * jax.random.uniform(streams_of[3], (NOBS,), jnp.float32) ** block_scale(streams_of[3], (NOBS,), ((0, 32),), -0.2, 0.2)), 0.5, 2.0)
    obs_patch = plant(jax.random.randint(streams_of[4], (NOBS,), 0, PD), jax.random.fold_in(streams_of[4], 1), 0, PD - 1).astype(jnp.int32)
    obs_position = plant(jax.random.randint(streams_of[5], (NOBS,), 0, 1073741824), jax.random.fold_in(streams_of[5], 1), 0, 1073741823).astype(jnp.int32)
    return {"background": background, "patch_blocks": patch_blocks, "obs_values": obs_values, "obs_errors": obs_errors, "obs_patch": obs_patch, "obs_position": obs_position}


neighbour_weight = 0.5

def inverse_root(system):
    precise = lax.Precision.HIGHEST
    identity = jnp.eye(K, dtype=jnp.float32)
    norm_value = jnp.sqrt(lax.optimization_barrier(jnp.sum(system * system, axis=(1, 2))))
    square_part = system / norm_value[:, None, None]
    inverse_part = jnp.broadcast_to(identity, system.shape)
    for sweep_index in range(NS_STEPS):
        middle = 1.5 * identity - 0.5 * jnp.einsum('pij,pjk->pik', inverse_part, square_part, precision=precise)
        square_part = jnp.einsum('pij,pjk->pik', square_part, middle, precision=precise)
        inverse_part = jnp.einsum('pij,pjk->pik', middle, inverse_part, precision=precise)
    return inverse_part / jnp.sqrt(norm_value)[:, None, None]

def localize(patch_field):
    zero_row = jnp.zeros_like(patch_field[:1])
    previous = jnp.concatenate([zero_row, patch_field[:-1]], axis=0)
    following = jnp.concatenate([patch_field[1:], zero_row], axis=0)
    return patch_field + neighbour_weight * (previous + following)

def reference(background, patch_blocks, obs_values, obs_errors, obs_patch, obs_position):
    precise = lax.Precision.HIGHEST
    patch_ids = jnp.arange(NOBS, dtype=jnp.int32) // OBS_DEV * PD + obs_patch
    used_blocks = patch_blocks[patch_ids]
    cell_index = obs_position % (used_blocks * CB)
    flat_index = patch_ids * (MAXB * CB) + cell_index
    thickness = jnp.transpose(background[:, :, 0], (0, 1, 3, 2)).reshape(NP * MAXB * CB, K)
    sampled = thickness[flat_index].astype(jnp.float32)
    obs_mean = lax.optimization_barrier(jnp.sum(sampled, axis=1)) / K
    spread = sampled - obs_mean[:, None]
    innovation = obs_values - obs_mean
    variance = lax.optimization_barrier(jnp.sum(spread * spread, axis=1)) / (K - 1)
    inflation = jnp.sum(innovation * innovation) / jnp.sum(variance + obs_errors * obs_errors)
    weighted = spread / obs_errors[:, None]
    scaled_innovation = innovation / obs_errors
    grouped_rows = weighted.reshape(N_PATCH, OBS_DEV, K)
    grouped_innovation = scaled_innovation.reshape(N_PATCH, OBS_DEV)
    grouped_slots = obs_patch.reshape(N_PATCH, OBS_DEV)

    def device_gram(operands):
        weight_rows, innov_rows, slot_rows = operands
        onehot = (slot_rows[None, :] == jnp.arange(PD, dtype=jnp.int32)[:, None]).astype(jnp.float32)
        masked = onehot[:, :, None] * weight_rows[None]
        gram_own = jnp.einsum('pjk,jl->pkl', masked, weight_rows, precision=precise)
        cross_own = jnp.einsum('pjk,j->pk', masked, innov_rows, precision=precise)
        return (gram_own, cross_own)
    gram_all, cross_all = lax.map(device_gram, (grouped_rows, grouped_innovation, grouped_slots))
    gram_all = localize(gram_all.reshape(NP, K, K))
    cross_all = localize(cross_all.reshape(NP, K))
    identity = jnp.eye(K, dtype=jnp.float32)
    system = (K - 1) / inflation * identity + gram_all
    root_inverse = inverse_root(system)
    inner_weights = jnp.einsum('pkl,pl->pk', root_inverse, cross_all, precision=precise)
    mean_weights = jnp.einsum('pkl,pl->pk', root_inverse, inner_weights, precision=precise)
    transform = (mean_weights[:, :, None] + math.sqrt(K - 1) * root_inverse).astype(jnp.bfloat16)
    transform = lax.optimization_barrier(transform)
    block_ids = jnp.arange(MAXB, dtype=jnp.int32)

    def update(operands):
        patch_state, weights, patch_used = operands
        member_mean = lax.optimization_barrier(jnp.sum(patch_state.astype(jnp.float32), axis=2)) / K
        anomaly = (patch_state.astype(jnp.float32) - member_mean[:, :, None, :]).astype(jnp.bfloat16)
        anomaly = lax.optimization_barrier(anomaly)
        combined = jnp.einsum('bvlc,lk->bvkc', anomaly.astype(jnp.float32), weights.astype(jnp.float32), precision=precise)
        in_use = (block_ids < patch_used)[:, None, None, None]
        result = jnp.where(in_use, member_mean[:, :, None, :] + combined, 0.0)
        return result.astype(jnp.bfloat16)
    analysis = lax.map(update, (background, transform, patch_blocks))
    return (analysis, inflation)
```

```python
import functools
import math

import jax
import jax.numpy as jnp
from jax import lax
from jax.experimental import pallas as pl
from jax.experimental.pallas import tpu as pltpu
from jax.sharding import PartitionSpec as P

K = 64
DEV_BLOCKS = 32
NS_STEPS = 4
neighbour_weight = 0.5
T_CHUNKS = 4
V_CHUNKS = 4
F32 = jnp.float32
BF16 = jnp.bfloat16


def split2(a):
    hi = a.astype(BF16)
    return hi, (a - hi.astype(F32)).astype(BF16)


def split3(a):
    hi = a.astype(BF16).astype(F32)
    rest = a - hi
    mid = rest.astype(BF16).astype(F32)
    return hi, mid, rest - mid


def dot_nn(a, b):
    return lax.dot_general(a, b, (((1,), (0,)), ((), ())), preferred_element_type=F32)


def dot_nt(a, b):
    return lax.dot_general(a, b, (((1,), (1,)), ((), ())), preferred_element_type=F32)


def product(a, b):
    n = a[0].shape[0]
    both = dot_nn(jnp.concatenate(a, axis=0), b[0])
    return both[:n] + both[n:] + dot_nn(a[0], b[1])


def total(a):
    return jnp.sum(jnp.sum(a, axis=0, keepdims=True), axis=1, keepdims=True)


def kernel(
    n_patch,
    n_member,
    used_ref,
    obs_ref,
    slot_patch_ref,
    position_ref,
    background_ref,
    out_ref,
    inflation_ref,
    own,
    tbuf,
    vbuf,
    obuf,
    wtab,
    mtab,
    ubuf,
    edge_send,
    edge_recv,
    sums,
    grams,
    roots,
    weights,
    defect,
    res,
    own_sem,
    t_send,
    t_recv,
    v_send,
    v_recv,
    o_send,
    o_recv,
    e_send,
    e_recv,
    s_send,
    s_recv,
):
    pd, maxb, nv, local, cb = own.shape
    me = lax.axis_index("member")
    pi = lax.axis_index("patch")
    near = me + 1 - 2 * (me % 2)
    far = (me + n_member // 2) % n_member
    cross = far + 1 - 2 * (far % 2)

    barrier = pltpu.get_barrier_semaphore()
    for peer in (near, far, cross):
        pl.semaphore_signal(
            barrier, inc=1, device_id={"member": peer}, device_id_type=pl.DeviceIdType.MESH
        )

    def greet(i, carry):
        peer = (pi + i) % n_patch
        pl.semaphore_signal(
            barrier, inc=1, device_id={"patch": peer}, device_id_type=pl.DeviceIdType.MESH
        )
        return carry

    lax.fori_loop(1, n_patch, greet, 0)
    load = pltpu.make_async_copy(background_ref, own, own_sem)
    load.start()

    used = [used_ref[pi * pd + p] for p in range(pd)]
    start = [jnp.int32(0)]
    for p in range(pd - 1):
        start.append(start[-1] + used[p])

    def patch_of(s):
        p = jnp.int32(0)
        first = jnp.int32(0)
        for q in range(1, pd):
            inside = s >= start[q]
            p = jnp.where(inside, q, p)
            first = jnp.where(inside, start[q], first)
        return p, jnp.minimum(s - first, maxb - 1)

    slot_patch = slot_patch_ref[...]
    position = position_ref[...]
    blocks = jnp.zeros_like(position)
    offset = jnp.zeros_like(position)
    for p in range(pd):
        blocks = jnp.where(slot_patch == p, used[p], blocks)
        offset = jnp.where(slot_patch == p, start[p], offset)
    lane = position & (cb - 1)
    quotient = position // cb
    blocks_f = blocks.astype(F32)
    rest = quotient - blocks * jnp.floor(quotient.astype(F32) / blocks_f).astype(jnp.int32)
    for _ in range(2):
        rest = jnp.where(rest < 0, rest + blocks, rest)
    for _ in range(2):
        rest = jnp.where(rest >= blocks, rest - blocks, rest)
    slot = offset + rest

    load.wait()
    per = DEV_BLOCKS // T_CHUNKS
    for s in range(DEV_BLOCKS):
        p, b = patch_of(s)
        x = own[p, b]
        tbuf[me, s] = x[0]
        vbuf[me, s] = x[1:]
    obuf[me] = obs_ref[...]

    pl.semaphore_wait(barrier, 3 + n_patch - 1)

    def remote(src, dst, send, recv, **where):
        return pltpu.make_async_remote_copy(
            src_ref=src,
            dst_ref=dst,
            send_sem=send,
            recv_sem=recv,
            device_id=where,
            device_id_type=pl.DeviceIdType.MESH,
        )

    def obs_copy(i, peer, holder):
        return remote(obs_ref, obuf.at[holder], o_send.at[i], o_recv.at[i], member=peer)

    def t_copy(route, c, peer, holder):
        part = tbuf.at[holder, pl.ds(c * per, per)]
        return remote(part, part, t_send.at[route, c], t_recv.at[route, c], member=peer)

    vper = DEV_BLOCKS // V_CHUNKS

    def v_copy(route, c, peer, holder):
        part = vbuf.at[holder, pl.ds(c * vper, vper)]
        return remote(part, part, v_send.at[route, c], v_recv.at[route, c], member=peer)

    for i, peer in enumerate((near, far, cross)):
        obs_copy(i, peer, me).start()
    for c in range(T_CHUNKS):
        t_copy(1, c, far, me).start()
    for c in range(T_CHUNKS):
        t_copy(0, c, near, me).start()
    for c in range(V_CHUNKS):
        v_copy(1, c, far, me).start()
    for c in range(V_CHUNKS):
        v_copy(0, c, near, me).start()

    for i, holder in enumerate((near, far, cross)):
        obs_copy(i, holder, holder).wait_recv()

    rows = DEV_BLOCKS
    n_obs_rows = position.shape[0]
    half = obs_ref.shape[0] // 2
    values = jnp.concatenate([obuf[m, :half] for m in range(n_member)], axis=0)
    errors = jnp.concatenate([obuf[m, half:] for m in range(n_member)], axis=0)
    inverse = 1.0 / (errors * errors)
    parts = [*split3(inverse), *split3(values * inverse), *split3(values), jnp.ones_like(values)]
    slot_rows = lax.broadcasted_iota(jnp.int32, (rows, cb), 0)
    lane_rows = lax.broadcasted_iota(jnp.int32, (cb, cb), 0)
    acc = jnp.zeros((len(parts) * rows, cb), F32)
    for r in range(0, n_obs_rows, 2):
        left, right = [], []
        for q in (r, r + 1):
            hit = slot_rows == slot[q : q + 1]
            left.append(
                jnp.concatenate(
                    [jnp.where(hit, part[q : q + 1], 0.0) for part in parts], axis=0
                ).astype(BF16)
            )
            right.append(jnp.where(lane_rows == lane[q : q + 1], 1.0, 0.0).astype(BF16))
        acc = acc + dot_nt(jnp.concatenate(left, axis=1), jnp.concatenate(right, axis=1))
    tables = [acc[i * rows : (i + 1) * rows] for i in range(len(parts))]
    weight = tables[0] + tables[1] + tables[2]
    pull = tables[3] + tables[4] + tables[5]
    number = tables[9]
    centre = (tables[6] + tables[7] + tables[8]) / jnp.maximum(number, 1.0)
    scale = jnp.sqrt(weight)
    inverse_scale = jnp.where(weight > 0.0, 1.0 / jnp.maximum(scale, 1e-6), 0.0)
    wtab[0] = scale
    wtab[1] = pull * inverse_scale
    centre_parts = jnp.concatenate(split3(centre), axis=0).astype(BF16)
    apart = jnp.zeros((1, cb), F32)
    for q in range(n_obs_rows):
        onehot = jnp.where(lane_rows == lane[q : q + 1], 1.0, 0.0).astype(BF16)
        found = dot_nn(centre_parts, onehot)
        found = found[:rows] + found[rows : 2 * rows] + found[2 * rows :]
        found = jnp.sum(
            jnp.where(slot_rows == slot[q : q + 1], found, 0.0), axis=0, keepdims=True
        )
        apart = apart + (values[q : q + 1] - found) ** 2
    apart = jnp.sum(apart, axis=1, keepdims=True)
    error_sum = total(errors * errors)

    part_row = lax.broadcasted_iota(jnp.int32, (16, cb), 0)

    def centre_chunk(c, carry):
        t_copy(1, c, far, far).wait_recv()
        t_copy(2, c, near, far).start()
        t_copy(0, c, near, near).wait_recv()
        t_copy(2, c, near, cross).wait_recv()
        for i in range(per):
            s = c * per + i
            x = jnp.concatenate([tbuf[m, s] for m in range(n_member)], axis=0).astype(F32)
            mean = jnp.sum(x, axis=0, keepdims=True) / K
            a = x - mean
            mtab[0, pl.ds(s, 1)] = mean
            mtab[1, pl.ds(s, 1)] = jnp.sum(a * a, axis=0, keepdims=True)
            row = wtab[0, pl.ds(s, 1)]
            hi, lo = split2(a * row)
            ubuf[s, :K] = hi
            ubuf[s, K : 2 * K] = lo
            v1, v2, v3 = split3(wtab[1, pl.ds(s, 1)] - mean * row)
            v = jnp.where(
                part_row == 0,
                v1,
                jnp.where(part_row == 1, v2, jnp.where(part_row == 2, v3, 0.0)),
            )
            ubuf[s, 2 * K :] = v.astype(BF16)
        return carry

    lax.fori_loop(0, T_CHUNKS, centre_chunk, 0)
    means = mtab[0]
    misfit = apart + total(number * (centre - means) ** 2)
    spread = error_sum + total(number * mtab[1]) / (K - 1)
    sum_rows = lax.broadcasted_iota(jnp.int32, (8, cb), 0)
    sums[pi] = jnp.where(sum_rows == 0, misfit, spread)

    def sum_copy(slot_index, peer):
        return remote(
            sums.at[slot_index],
            sums.at[slot_index],
            s_send.at[peer],
            s_recv.at[slot_index],
            patch=peer,
        )

    def send_sum(i, carry):
        sum_copy(pi, (pi + i) % n_patch).start()
        return carry

    lax.fori_loop(1, n_patch, send_sum, 0)

    def gram_of(p):
        acc = jnp.zeros((2 * K + 16, 2 * K), F32)
        for b in range(0, maxb, 2):
            pair = []
            for q in (b, b + 1):
                u = ubuf[jnp.minimum(start[p] + q, DEV_BLOCKS - 1)]
                pair.append(jnp.where(q < used[p], u, jnp.zeros_like(u)))
            pair = jnp.concatenate(pair, axis=1)
            acc = acc + dot_nt(pair, pair[: 2 * K])
        g = acc[:K] + acc[K : 2 * K]
        c = jnp.broadcast_to(jnp.sum(acc[2 * K :], axis=0, keepdims=True), (8, 2 * K))
        full = jnp.concatenate([g, c], axis=0)
        return full + pltpu.roll(full, K, 1)

    def edge_copy(i, peer):
        return remote(edge_send.at[i], edge_recv.at[i], e_send.at[i], e_recv.at[i], patch=peer)

    up = (pi + 1) % n_patch
    down = (pi + n_patch - 1) % n_patch
    gram = [None] * pd
    gram[pd - 1] = gram_of(pd - 1)
    edge_send[0] = gram[pd - 1]
    gram[0] = gram_of(0)
    edge_send[1] = gram[0]

    @pl.when(pi < n_patch - 1)
    def _():
        edge_copy(0, up).start()

    @pl.when(pi > 0)
    def _():
        edge_copy(1, down).start()

    for p in range(1, pd - 1):
        gram[p] = gram_of(p)
    for p in range(pd):
        grams[p] = gram[p]

    def relay(c, carry):
        v_copy(1, c, far, far).wait_recv()
        v_copy(2, c, near, far).start()
        return carry

    lax.fori_loop(0, V_CHUNKS, relay, 0)

    @pl.when(pi > 0)
    def _():
        edge_copy(0, up).wait_recv()

    @pl.when(pi == 0)
    def _():
        edge_recv[0] = jnp.zeros(edge_recv.shape[1:], F32)

    @pl.when(pi < n_patch - 1)
    def _():
        edge_copy(1, down).wait_recv()

    @pl.when(pi == n_patch - 1)
    def _():
        edge_recv[1] = jnp.zeros(edge_recv.shape[1:], F32)

    def recv_sum(i, carry):
        peer = (pi + i) % n_patch
        sum_copy(peer, peer).wait_recv()
        return carry

    lax.fori_loop(1, n_patch, recv_sum, 0)
    both = jnp.sum(sums[...], axis=0)
    inflation = both[0:1] / both[1:2]
    inflation_ref[...] = jnp.broadcast_to(inflation, inflation_ref.shape)

    eye = jnp.where(
        lax.broadcasted_iota(jnp.int32, (K, K), 0) == lax.broadcasted_iota(jnp.int32, (K, K), 1),
        1.0,
        0.0,
    )
    field = [edge_recv[0]] + [grams[p] for p in range(pd)] + [edge_recv[1]]
    ridge = (K - 1) / inflation[:, :K]
    square, norm, drive = [], [], []
    for p in range(pd):
        local_field = field[p + 1] + neighbour_weight * (field[p] + field[p + 2])
        system = local_field[:K, :K] + ridge * eye
        drive.append(local_field[K : K + 1, :K])
        size = jnp.sqrt(total(system * system))
        norm.append(size)
        square.append(system / size)
    middle = [1.5 * eye - 0.5 * a for a in square]
    inverse_part = middle
    m_parts = [split2(a) for a in middle]
    z_parts = m_parts
    s_parts = [split2(a) for a in square]
    for sweep in range(1, NS_STEPS):
        square = [product(a, b) for a, b in zip(s_parts, m_parts)]
        s_parts = [split2(a) for a in square]
        middle = [1.5 * eye - 0.5 * product(a, b) for a, b in zip(z_parts, s_parts)]
        m_parts = [split2(a) for a in middle]
        inverse_part = [product(a, b) for a, b in zip(m_parts, z_parts)]
        z_parts = [split2(a) for a in inverse_part]
    for p in range(pd):
        root = inverse_part[p] / jnp.sqrt(norm[p])
        inner = jnp.sum(root * drive[p], axis=1, keepdims=True)
        mean_weights = jnp.sum(root * inner, axis=0, keepdims=True)
        roots[p] = mean_weights + math.sqrt(K - 1) * root
        mine = roots[p, pl.ds(me * local, local)].astype(BF16)
        weights[p, :local] = mine
        weights[p, local:] = jnp.ones((16, K), BF16)
        short = (1.0 - jnp.sum(mine.astype(F32), axis=1, keepdims=True)) / K
        defect[p] = jnp.broadcast_to(short, (local, cb))

    def finish_chunk(c, carry):
        v_copy(0, c, near, near).wait_recv()
        v_copy(2, c, near, cross).wait_recv()
        for i in range(vper):
            s = c * vper + i
            p, _ = patch_of(s)
            w = weights[p]
            d = defect[p]
            thick = jnp.concatenate([tbuf[m, s] for m in range(n_member)], axis=0)
            speeds = [
                jnp.concatenate([vbuf[m, s, v] for m in range(n_member)], axis=0)
                for v in range(nv - 1)
            ]
            got = dot_nn(w, jnp.concatenate([thick] + speeds, axis=1))
            for v in range(nv):
                g = got[:, v * cb : (v + 1) * cb]
                res[s, v] = (g[:local] + g[local : local + 1] * d).astype(BF16)
        return carry

    lax.fori_loop(0, V_CHUNKS, finish_chunk, 0)

    for p in range(pd):
        for b in range(maxb):
            r = res[jnp.minimum(start[p] + b, DEV_BLOCKS - 1)]
            out_ref[p, b] = jnp.where(b < used[p], r, jnp.zeros_like(r))

    for i, peer in enumerate((near, far, cross)):
        obs_copy(i, peer, me).wait_send()
    for c in range(T_CHUNKS):
        t_copy(0, c, near, me).wait_send()
        t_copy(1, c, far, me).wait_send()
        t_copy(2, c, near, far).wait_send()
    for c in range(V_CHUNKS):
        v_copy(0, c, near, me).wait_send()
        v_copy(1, c, far, me).wait_send()
        v_copy(2, c, near, far).wait_send()

    @pl.when(pi < n_patch - 1)
    def _():
        edge_copy(0, up).wait_send()

    @pl.when(pi > 0)
    def _():
        edge_copy(1, down).wait_send()

    def sum_left(i, carry):
        sum_copy(pi, (pi + i) % n_patch).wait_send()
        return carry

    lax.fori_loop(1, n_patch, sum_left, 0)


def solution(mesh):
    n_patch, n_member = mesh.shape["patch"], mesh.shape["member"]

    def per_device(background, patch_blocks, obs_values, obs_errors, obs_patch, obs_position):
        pd, maxb, nv, local, cb = background.shape
        obs = jnp.concatenate([obs_values.reshape(-1, cb), obs_errors.reshape(-1, cb)], axis=0)
        vmem = pl.BlockSpec(memory_space=pltpu.VMEM)
        dma = pltpu.SemaphoreType.DMA
        analysis, inflation = pl.pallas_call(
            functools.partial(kernel, n_patch, n_member),
            out_shape=(
                jax.ShapeDtypeStruct(background.shape, BF16),
                jax.ShapeDtypeStruct((8, cb), F32),
            ),
            in_specs=[
                pl.BlockSpec(memory_space=pltpu.SMEM),
                vmem,
                vmem,
                vmem,
                pl.BlockSpec(memory_space=pl.ANY),
            ],
            out_specs=(vmem, vmem),
            scratch_shapes=[
                pltpu.VMEM(background.shape, BF16),
                pltpu.VMEM((n_member, DEV_BLOCKS, local, cb), BF16),
                pltpu.VMEM((n_member, DEV_BLOCKS, nv - 1, local, cb), BF16),
                pltpu.VMEM((n_member, *obs.shape), F32),
                pltpu.VMEM((2, DEV_BLOCKS, cb), F32),
                pltpu.VMEM((2, DEV_BLOCKS, cb), F32),
                pltpu.VMEM((DEV_BLOCKS, 2 * K + 16, cb), BF16),
                pltpu.VMEM((2, K + 8, 2 * K), F32),
                pltpu.VMEM((2, K + 8, 2 * K), F32),
                pltpu.VMEM((n_patch, 8, cb), F32),
                pltpu.VMEM((pd, K + 8, 2 * K), F32),
                pltpu.VMEM((pd, K, K), F32),
                pltpu.VMEM((pd, local + 16, K), BF16),
                pltpu.VMEM((pd, local, cb), F32),
                pltpu.VMEM((DEV_BLOCKS, nv, local, cb), BF16),
                dma,
                dma((3, T_CHUNKS)),
                dma((3, T_CHUNKS)),
                dma((3, V_CHUNKS)),
                dma((3, V_CHUNKS)),
                dma((3,)),
                dma((3,)),
                dma((2,)),
                dma((2,)),
                dma((n_patch,)),
                dma((n_patch,)),
            ],
            compiler_params=pltpu.CompilerParams(collective_id=0, has_side_effects=True),
        )(
            patch_blocks,
            obs,
            obs_patch.reshape(-1, cb),
            obs_position.reshape(-1, cb),
            background,
        )
        return analysis, inflation[0, 0]

    in_specs = (
        P("patch", None, None, "member", None),
        P(),
        P(("patch", "member")),
        P(("patch", "member")),
        P("patch"),
        P("patch"),
    )
    out_specs = (P("patch", None, None, "member", None), P())
    return jax.shard_map(
        per_device, mesh=mesh, in_specs=in_specs, out_specs=out_specs, check_vma=False
    )
```

```python
import functools
import math

import jax
import jax.numpy as jnp
from jax import lax
from jax.experimental import pallas as pl
from jax.experimental.pallas import tpu as pltpu
from jax.sharding import PartitionSpec as P

K = 64
DEV_BLOCKS = 32
NS_STEPS = 4
neighbour_weight = 0.5
T_CHUNKS = 4
V_CHUNKS = 4
F32 = jnp.float32
BF16 = jnp.bfloat16


def split2(a):
    hi = a.astype(BF16)
    return hi, (a - hi.astype(F32)).astype(BF16)


def split3(a):
    hi = a.astype(BF16).astype(F32)
    rest = a - hi
    mid = rest.astype(BF16).astype(F32)
    return hi, mid, rest - mid


def dot_nn(a, b):
    return lax.dot_general(a, b, (((1,), (0,)), ((), ())), preferred_element_type=F32)


def dot_nt(a, b):
    return lax.dot_general(a, b, (((1,), (1,)), ((), ())), preferred_element_type=F32)


def product(a, b):
    n = a[0].shape[0]
    both = dot_nn(jnp.concatenate(a, axis=0), b[0])
    return both[:n] + both[n:] + dot_nn(a[0], b[1])


def total(a):
    return jnp.sum(jnp.sum(a, axis=0, keepdims=True), axis=1, keepdims=True)


def kernel(
    n_patch,
    n_member,
    used_ref,
    values_ref,
    errors_ref,
    slot_patch_hbm,
    position_hbm,
    background_ref,
    res,
    inflation_ref,
    own,
    obs_ref,
    slot_patch_ref,
    position_ref,
    tbuf,
    vbuf,
    obuf,
    wtab,
    mtab,
    ubuf,
    edge_send,
    edge_recv,
    sums,
    grams,
    roots,
    weights,
    defect,
    own_sem,
    in_sem,
    t_send,
    t_recv,
    v_send,
    v_recv,
    o_send,
    o_recv,
    e_send,
    e_recv,
    s_send,
    s_recv,
):
    pd, maxb, nv, local, cb = own.shape
    me = lax.axis_index("member")
    pi = lax.axis_index("patch")
    near = me + 1 - 2 * (me % 2)
    far = (me + n_member // 2) % n_member
    cross = far + 1 - 2 * (far % 2)

    barrier = pltpu.get_barrier_semaphore()
    for peer in (near, far, cross):
        pl.semaphore_signal(
            barrier, inc=1, device_id={"member": peer}, device_id_type=pl.DeviceIdType.MESH
        )

    def greet(i, carry):
        peer = (pi + i) % n_patch
        pl.semaphore_signal(
            barrier, inc=1, device_id={"patch": peer}, device_id_type=pl.DeviceIdType.MESH
        )
        return carry

    lax.fori_loop(1, n_patch, greet, 0)
    small = [
        pltpu.make_async_copy(source, target, in_sem.at[i])
        for i, (source, target) in enumerate(
            (
                (values_ref, obs_ref.at[0]),
                (errors_ref, obs_ref.at[1]),
                (slot_patch_hbm, slot_patch_ref),
                (position_hbm, position_ref),
            )
        )
    ]
    for copy in small:
        copy.start()
    load = pltpu.make_async_copy(background_ref, own, own_sem)
    load.start()

    used = [used_ref[pi * pd + p] for p in range(pd)]
    start = [jnp.int32(0)]
    for p in range(pd - 1):
        start.append(start[-1] + used[p])

    def patch_of(s):
        p = jnp.int32(0)
        first = jnp.int32(0)
        for q in range(1, pd):
            inside = s >= start[q]
            p = jnp.where(inside, q, p)
            first = jnp.where(inside, start[q], first)
        return p, jnp.minimum(s - first, maxb - 1)

    for copy in small:
        copy.wait()
    slot_patch = slot_patch_ref[...]
    position = position_ref[...]
    blocks = jnp.zeros_like(position)
    offset = jnp.zeros_like(position)
    for p in range(pd):
        blocks = jnp.where(slot_patch == p, used[p], blocks)
        offset = jnp.where(slot_patch == p, start[p], offset)
    lane = position & (cb - 1)
    quotient = position // cb
    blocks_f = blocks.astype(F32)
    rest = quotient - blocks * jnp.floor(quotient.astype(F32) / blocks_f).astype(jnp.int32)
    for _ in range(2):
        rest = jnp.where(rest < 0, rest + blocks, rest)
    for _ in range(2):
        rest = jnp.where(rest >= blocks, rest - blocks, rest)
    slot = offset + rest

    load.wait()
    per = DEV_BLOCKS // T_CHUNKS
    for s in range(DEV_BLOCKS):
        p, b = patch_of(s)
        x = own[p, b]
        tbuf[me, s] = x[0]
        vbuf[me, s] = x[1:]
    obuf[me] = obs_ref[...]

    pl.semaphore_wait(barrier, 3 + n_patch - 1)

    def remote(src, dst, send, recv, **where):
        return pltpu.make_async_remote_copy(
            src_ref=src,
            dst_ref=dst,
            send_sem=send,
            recv_sem=recv,
            device_id=where,
            device_id_type=pl.DeviceIdType.MESH,
        )

    def obs_copy(i, peer, holder):
        return remote(obs_ref, obuf.at[holder], o_send.at[i], o_recv.at[i], member=peer)

    def t_copy(route, c, peer, holder):
        part = tbuf.at[holder, pl.ds(c * per, per)]
        return remote(part, part, t_send.at[route, c], t_recv.at[route, c], member=peer)

    vper = DEV_BLOCKS // V_CHUNKS

    def v_copy(route, c, peer, holder):
        part = vbuf.at[holder, pl.ds(c * vper, vper)]
        return remote(part, part, v_send.at[route, c], v_recv.at[route, c], member=peer)

    for i, peer in enumerate((near, far, cross)):
        obs_copy(i, peer, me).start()
    for c in range(T_CHUNKS):
        t_copy(1, c, far, me).start()
    for c in range(T_CHUNKS):
        t_copy(0, c, near, me).start()
    for c in range(V_CHUNKS):
        v_copy(1, c, far, me).start()
    for c in range(V_CHUNKS):
        v_copy(0, c, near, me).start()

    for i, holder in enumerate((near, far, cross)):
        obs_copy(i, holder, holder).wait_recv()

    rows = DEV_BLOCKS
    n_obs_rows = position.shape[0]
    values = jnp.concatenate([obuf[m, 0] for m in range(n_member)], axis=0)
    errors = jnp.concatenate([obuf[m, 1] for m in range(n_member)], axis=0)
    inverse = 1.0 / (errors * errors)
    parts = [*split3(inverse), *split3(values * inverse), *split3(values), jnp.ones_like(values)]
    slot_rows = lax.broadcasted_iota(jnp.int32, (rows, cb), 0)
    lane_rows = lax.broadcasted_iota(jnp.int32, (cb, cb), 0)
    acc = jnp.zeros((len(parts) * rows, cb), F32)
    for r in range(0, n_obs_rows, 2):
        left, right = [], []
        for q in (r, r + 1):
            hit = slot_rows == slot[q : q + 1]
            left.append(
                jnp.concatenate(
                    [jnp.where(hit, part[q : q + 1], 0.0) for part in parts], axis=0
                ).astype(BF16)
            )
            right.append(jnp.where(lane_rows == lane[q : q + 1], 1.0, 0.0).astype(BF16))
        acc = acc + dot_nt(jnp.concatenate(left, axis=1), jnp.concatenate(right, axis=1))
    tables = [acc[i * rows : (i + 1) * rows] for i in range(len(parts))]
    weight = tables[0] + tables[1] + tables[2]
    pull = tables[3] + tables[4] + tables[5]
    number = tables[9]
    centre = (tables[6] + tables[7] + tables[8]) / jnp.maximum(number, 1.0)
    scale = jnp.sqrt(weight)
    inverse_scale = jnp.where(weight > 0.0, 1.0 / jnp.maximum(scale, 1e-6), 0.0)
    wtab[0] = scale
    wtab[1] = pull * inverse_scale
    centre_parts = jnp.concatenate(split3(centre), axis=0).astype(BF16)
    apart = jnp.zeros((1, cb), F32)
    for q in range(n_obs_rows):
        onehot = jnp.where(lane_rows == lane[q : q + 1], 1.0, 0.0).astype(BF16)
        found = dot_nn(centre_parts, onehot)
        found = found[:rows] + found[rows : 2 * rows] + found[2 * rows :]
        found = jnp.sum(
            jnp.where(slot_rows == slot[q : q + 1], found, 0.0), axis=0, keepdims=True
        )
        apart = apart + (values[q : q + 1] - found) ** 2
    apart = jnp.sum(apart, axis=1, keepdims=True)
    error_sum = total(errors * errors)

    part_row = lax.broadcasted_iota(jnp.int32, (16, cb), 0)

    def forward(c):
        t_copy(1, c, far, far).wait_recv()
        t_copy(2, c, near, far).start()

    forward(0)

    def centre_chunk(c, carry):
        @pl.when(c + 1 < T_CHUNKS)
        def _():
            forward(c + 1)

        t_copy(0, c, near, near).wait_recv()
        t_copy(2, c, near, cross).wait_recv()
        for i in range(per):
            s = c * per + i
            x = jnp.concatenate([tbuf[m, s] for m in range(n_member)], axis=0).astype(F32)
            mean = jnp.sum(x, axis=0, keepdims=True) / K
            a = x - mean
            mtab[0, pl.ds(s, 1)] = mean
            mtab[1, pl.ds(s, 1)] = jnp.sum(a * a, axis=0, keepdims=True)
            row = wtab[0, pl.ds(s, 1)]
            hi, lo = split2(a * row)
            ubuf[s, :K] = hi
            ubuf[s, K : 2 * K] = lo
            v1, v2, v3 = split3(wtab[1, pl.ds(s, 1)] - mean * row)
            v = jnp.where(
                part_row == 0,
                v1,
                jnp.where(part_row == 1, v2, jnp.where(part_row == 2, v3, 0.0)),
            )
            ubuf[s, 2 * K :] = v.astype(BF16)
        return carry

    lax.fori_loop(0, T_CHUNKS, centre_chunk, 0)
    means = mtab[0]
    misfit = apart + total(number * (centre - means) ** 2)
    spread = error_sum + total(number * mtab[1]) / (K - 1)
    sum_rows = lax.broadcasted_iota(jnp.int32, (8, cb), 0)
    sums[pi] = jnp.where(sum_rows == 0, misfit, spread)

    def sum_copy(slot_index, peer):
        return remote(
            sums.at[slot_index],
            sums.at[slot_index],
            s_send.at[peer],
            s_recv.at[slot_index],
            patch=peer,
        )

    def send_sum(i, carry):
        sum_copy(pi, (pi + i) % n_patch).start()
        return carry

    lax.fori_loop(1, n_patch, send_sum, 0)

    def gram_of(p):
        acc = jnp.zeros((2 * K + 16, 2 * K), F32)
        for b in range(0, maxb, 2):
            pair = []
            for q in (b, b + 1):
                u = ubuf[jnp.minimum(start[p] + q, DEV_BLOCKS - 1)]
                pair.append(jnp.where(q < used[p], u, jnp.zeros_like(u)))
            pair = jnp.concatenate(pair, axis=1)
            acc = acc + dot_nt(pair, pair[: 2 * K])
        g = acc[:K] + acc[K : 2 * K]
        c = jnp.broadcast_to(jnp.sum(acc[2 * K :], axis=0, keepdims=True), (8, 2 * K))
        full = jnp.concatenate([g, c], axis=0)
        return full + pltpu.roll(full, K, 1)

    def edge_copy(i, peer):
        return remote(edge_send.at[i], edge_recv.at[i], e_send.at[i], e_recv.at[i], patch=peer)

    up = (pi + 1) % n_patch
    down = (pi + n_patch - 1) % n_patch
    gram = [None] * pd
    gram[pd - 1] = gram_of(pd - 1)
    edge_send[0] = gram[pd - 1]
    gram[0] = gram_of(0)
    edge_send[1] = gram[0]

    @pl.when(pi < n_patch - 1)
    def _():
        edge_copy(0, up).start()

    @pl.when(pi > 0)
    def _():
        edge_copy(1, down).start()

    for p in range(1, pd - 1):
        gram[p] = gram_of(p)
    for p in range(pd):
        grams[p] = gram[p]

    def relay(c, carry):
        v_copy(1, c, far, far).wait_recv()
        v_copy(2, c, near, far).start()
        return carry

    lax.fori_loop(0, V_CHUNKS, relay, 0)

    @pl.when(pi > 0)
    def _():
        edge_copy(0, up).wait_recv()

    @pl.when(pi == 0)
    def _():
        edge_recv[0] = jnp.zeros(edge_recv.shape[1:], F32)

    @pl.when(pi < n_patch - 1)
    def _():
        edge_copy(1, down).wait_recv()

    @pl.when(pi == n_patch - 1)
    def _():
        edge_recv[1] = jnp.zeros(edge_recv.shape[1:], F32)

    def recv_sum(i, carry):
        peer = (pi + i) % n_patch
        sum_copy(peer, peer).wait_recv()
        return carry

    lax.fori_loop(1, n_patch, recv_sum, 0)
    both = jnp.sum(sums[...], axis=0)
    inflation = both[0:1] / both[1:2]
    inflation_ref[0, 0] = jnp.max(inflation)

    eye = jnp.where(
        lax.broadcasted_iota(jnp.int32, (K, K), 0) == lax.broadcasted_iota(jnp.int32, (K, K), 1),
        1.0,
        0.0,
    )
    field = [edge_recv[0]] + [grams[p] for p in range(pd)] + [edge_recv[1]]
    ridge = (K - 1) / inflation[:, :K]
    square, norm, drive = [], [], []
    for p in range(pd):
        local_field = field[p + 1] + neighbour_weight * (field[p] + field[p + 2])
        system = local_field[:K, :K] + ridge * eye
        drive.append(local_field[K : K + 1, :K])
        size = jnp.sqrt(total(system * system))
        norm.append(size)
        square.append(system / size)
    middle = [1.5 * eye - 0.5 * a for a in square]
    inverse_part = middle
    m_parts = [split2(a) for a in middle]
    z_parts = m_parts
    s_parts = [split2(a) for a in square]
    for sweep in range(1, NS_STEPS):
        square = [product(a, b) for a, b in zip(s_parts, m_parts)]
        s_parts = [split2(a) for a in square]
        middle = [1.5 * eye - 0.5 * product(a, b) for a, b in zip(z_parts, s_parts)]
        m_parts = [split2(a) for a in middle]
        inverse_part = [product(a, b) for a, b in zip(m_parts, z_parts)]
        z_parts = [split2(a) for a in inverse_part]
    for p in range(pd):
        root = inverse_part[p] / jnp.sqrt(norm[p])
        inner = jnp.sum(root * drive[p], axis=1, keepdims=True)
        mean_weights = jnp.sum(root * inner, axis=0, keepdims=True)
        roots[p] = mean_weights + math.sqrt(K - 1) * root
        mine = roots[p, pl.ds(me * local, local)].astype(BF16)
        weights[p, :local] = mine
        weights[p, local:] = jnp.ones((16, K), BF16)
        short = (1.0 - jnp.sum(mine.astype(F32), axis=1, keepdims=True)) / K
        defect[p] = jnp.broadcast_to(short, (local, cb))

    def finish_chunk(c, carry):
        v_copy(0, c, near, near).wait_recv()
        v_copy(2, c, near, cross).wait_recv()
        for i in range(vper):
            s = c * vper + i
            p, _ = patch_of(s)
            w = weights[p]
            d = defect[p]
            thick = jnp.concatenate([tbuf[m, s] for m in range(n_member)], axis=0)
            speeds = [
                jnp.concatenate([vbuf[m, s, v] for m in range(n_member)], axis=0)
                for v in range(nv - 1)
            ]
            got = dot_nn(w, jnp.concatenate([thick] + speeds, axis=1))
            for v in range(nv):
                g = got[:, v * cb : (v + 1) * cb]
                res[s, v] = (g[:local] + g[local : local + 1] * d).astype(BF16)
        return carry

    lax.fori_loop(0, V_CHUNKS, finish_chunk, 0)

    for i, peer in enumerate((near, far, cross)):
        obs_copy(i, peer, me).wait_send()
    for c in range(T_CHUNKS):
        t_copy(0, c, near, me).wait_send()
        t_copy(1, c, far, me).wait_send()
        t_copy(2, c, near, far).wait_send()
    for c in range(V_CHUNKS):
        v_copy(0, c, near, me).wait_send()
        v_copy(1, c, far, me).wait_send()
        v_copy(2, c, near, far).wait_send()

    @pl.when(pi < n_patch - 1)
    def _():
        edge_copy(0, up).wait_send()

    @pl.when(pi > 0)
    def _():
        edge_copy(1, down).wait_send()

    def sum_left(i, carry):
        sum_copy(pi, (pi + i) % n_patch).wait_send()
        return carry

    lax.fori_loop(1, n_patch, sum_left, 0)


def expand_kernel(pd, used_ref, inflation_in, res, out_ref, inflation_out):
    p = pl.program_id(0)
    first = lax.axis_index("patch") * pd
    start = jnp.int32(0)
    for q in range(pd):
        start = start + jnp.where(q < p, used_ref[first + q], 0)
    used = used_ref[first + p]
    for b in range(out_ref.shape[1]):
        r = res[jnp.minimum(start + b, DEV_BLOCKS - 1)]
        out_ref[0, b] = jnp.where(b < used, r, jnp.zeros_like(r))
    inflation_out[0, 0] = inflation_in[0, 0]


def solution(mesh):
    n_patch, n_member = mesh.shape["patch"], mesh.shape["member"]

    def per_device(background, patch_blocks, obs_values, obs_errors, obs_patch, obs_position):
        pd, maxb, nv, local, cb = background.shape
        values, errors = obs_values.reshape(-1, cb), obs_errors.reshape(-1, cb)
        slot_patch, position = obs_patch.reshape(-1, cb), obs_position.reshape(-1, cb)
        vmem = pl.BlockSpec(memory_space=pltpu.VMEM)
        smem = pl.BlockSpec(memory_space=pltpu.SMEM)
        hbm = pl.BlockSpec(memory_space=pl.ANY)
        dma = pltpu.SemaphoreType.DMA
        packed, ratio = pl.pallas_call(
            functools.partial(kernel, n_patch, n_member),
            out_shape=(
                jax.ShapeDtypeStruct((DEV_BLOCKS, nv, local, cb), BF16),
                jax.ShapeDtypeStruct((1, 1), F32),
            ),
            in_specs=[
                smem,
                hbm,
                hbm,
                hbm,
                hbm,
                hbm,
            ],
            out_specs=(vmem, smem),
            scratch_shapes=[
                pltpu.VMEM(background.shape, BF16),
                pltpu.VMEM((2, *values.shape), F32),
                pltpu.VMEM(slot_patch.shape, jnp.int32),
                pltpu.VMEM(position.shape, jnp.int32),
                pltpu.VMEM((n_member, DEV_BLOCKS, local, cb), BF16),
                pltpu.VMEM((n_member, DEV_BLOCKS, nv - 1, local, cb), BF16),
                pltpu.VMEM((n_member, 2, *values.shape), F32),
                pltpu.VMEM((2, DEV_BLOCKS, cb), F32),
                pltpu.VMEM((2, DEV_BLOCKS, cb), F32),
                pltpu.VMEM((DEV_BLOCKS, 2 * K + 16, cb), BF16),
                pltpu.VMEM((2, K + 8, 2 * K), F32),
                pltpu.VMEM((2, K + 8, 2 * K), F32),
                pltpu.VMEM((n_patch, 8, cb), F32),
                pltpu.VMEM((pd, K + 8, 2 * K), F32),
                pltpu.VMEM((pd, K, K), F32),
                pltpu.VMEM((pd, local + 16, K), BF16),
                pltpu.VMEM((pd, local, cb), F32),
                dma,
                dma((4,)),
                dma((3, T_CHUNKS)),
                dma((3, T_CHUNKS)),
                dma((3, V_CHUNKS)),
                dma((3, V_CHUNKS)),
                dma((3,)),
                dma((3,)),
                dma((2,)),
                dma((2,)),
                dma((n_patch,)),
                dma((n_patch,)),
            ],
            compiler_params=pltpu.CompilerParams(collective_id=0, has_side_effects=True),
        )(
            patch_blocks,
            values,
            errors,
            slot_patch,
            position,
            background,
        )
        analysis, inflation = pl.pallas_call(
            functools.partial(expand_kernel, pd),
            grid=(pd,),
            out_shape=(
                jax.ShapeDtypeStruct(background.shape, BF16),
                jax.ShapeDtypeStruct((1, 1), F32),
            ),
            in_specs=[smem, smem, vmem],
            out_specs=(
                pl.BlockSpec((1, maxb, nv, local, cb), lambda p: (p, 0, 0, 0, 0)),
                smem,
            ),
        )(patch_blocks, ratio, packed)
        return analysis, inflation.reshape(())

    in_specs = (
        P("patch", None, None, "member", None),
        P(),
        P(("patch", "member")),
        P(("patch", "member")),
        P("patch"),
        P("patch"),
    )
    out_specs = (P("patch", None, None, "member", None), P())
    return jax.shard_map(
        per_device, mesh=mesh, in_specs=in_specs, out_specs=out_specs, check_vma=False
    )
```

```python
import functools
import math

import jax
import jax.numpy as jnp
from jax import lax
from jax.experimental import pallas as pl
from jax.experimental.pallas import tpu as pltpu
from jax.sharding import PartitionSpec as P

K = 64
DEV_BLOCKS = 32
NS_STEPS = 4
neighbour_weight = 0.5
T_CHUNKS = 4
V_CHUNKS = 2
F32 = jnp.float32
BF16 = jnp.bfloat16


def split2(a):
    hi = a.astype(BF16)
    return hi, (a - hi.astype(F32)).astype(BF16)


def split3(a):
    hi = a.astype(BF16).astype(F32)
    rest = a - hi
    mid = rest.astype(BF16).astype(F32)
    return hi, mid, rest - mid


def dot_nn(a, b):
    return lax.dot_general(a, b, (((1,), (0,)), ((), ())), preferred_element_type=F32)


def dot_nt(a, b):
    return lax.dot_general(a, b, (((1,), (1,)), ((), ())), preferred_element_type=F32)


def product(a, b):
    n = a[0].shape[0]
    both = dot_nn(jnp.concatenate(a, axis=0), b[0])
    return both[:n] + both[n:] + dot_nn(a[0], b[1])


def total(a):
    return jnp.sum(jnp.sum(a, axis=0, keepdims=True), axis=1, keepdims=True)


def kernel(
    n_patch,
    n_member,
    used_ref,
    values_ref,
    errors_ref,
    slot_patch_hbm,
    position_hbm,
    background_ref,
    res,
    inflation_ref,
    own,
    obs_ref,
    slot_patch_ref,
    position_ref,
    tbuf,
    vbuf,
    obuf,
    wtab,
    mtab,
    ubuf,
    edge_send,
    edge_recv,
    sums,
    grams,
    roots,
    weights,
    defect,
    own_sem,
    in_sem,
    t_send,
    t_recv,
    v_send,
    v_recv,
    o_send,
    o_recv,
    e_send,
    e_recv,
    s_send,
    s_recv,
):
    pd, maxb, nv, local, cb = own.shape
    me = lax.axis_index("member")
    pi = lax.axis_index("patch")
    near = me + 1 - 2 * (me % 2)
    far = (me + n_member // 2) % n_member
    cross = far + 1 - 2 * (far % 2)

    barrier = pltpu.get_barrier_semaphore()
    for peer in (near, far, cross):
        pl.semaphore_signal(
            barrier, inc=1, device_id={"member": peer}, device_id_type=pl.DeviceIdType.MESH
        )

    def greet(i, carry):
        peer = (pi + i) % n_patch
        pl.semaphore_signal(
            barrier, inc=1, device_id={"patch": peer}, device_id_type=pl.DeviceIdType.MESH
        )
        return carry

    lax.fori_loop(1, n_patch, greet, 0)
    small = [
        pltpu.make_async_copy(source, target, in_sem.at[i])
        for i, (source, target) in enumerate(
            (
                (values_ref, obs_ref.at[0]),
                (errors_ref, obs_ref.at[1]),
                (slot_patch_hbm, slot_patch_ref),
                (position_hbm, position_ref),
            )
        )
    ]
    for copy in small:
        copy.start()
    load = pltpu.make_async_copy(background_ref, own, own_sem)
    load.start()

    used = [used_ref[pi * pd + p] for p in range(pd)]
    start = [jnp.int32(0)]
    for p in range(pd - 1):
        start.append(start[-1] + used[p])

    def patch_of(s):
        p = jnp.int32(0)
        first = jnp.int32(0)
        for q in range(1, pd):
            inside = s >= start[q]
            p = jnp.where(inside, q, p)
            first = jnp.where(inside, start[q], first)
        return p, jnp.minimum(s - first, maxb - 1)

    for copy in small:
        copy.wait()
    slot_patch = slot_patch_ref[...]
    position = position_ref[...]
    blocks = jnp.zeros_like(position)
    offset = jnp.zeros_like(position)
    for p in range(pd):
        blocks = jnp.where(slot_patch == p, used[p], blocks)
        offset = jnp.where(slot_patch == p, start[p], offset)
    lane = position & (cb - 1)
    quotient = position // cb
    blocks_f = blocks.astype(F32)
    rest = quotient - blocks * jnp.floor(quotient.astype(F32) / blocks_f).astype(jnp.int32)
    for _ in range(2):
        rest = jnp.where(rest < 0, rest + blocks, rest)
    for _ in range(2):
        rest = jnp.where(rest >= blocks, rest - blocks, rest)
    slot = offset + rest

    load.wait()
    per = DEV_BLOCKS // T_CHUNKS
    for s in range(DEV_BLOCKS):
        p, b = patch_of(s)
        x = own[p, b]
        tbuf[me, s] = x[0]
        vbuf[me, s] = x[1:]
    obuf[me] = obs_ref[...]

    pl.semaphore_wait(barrier, 3 + n_patch - 1)

    def remote(src, dst, send, recv, **where):
        return pltpu.make_async_remote_copy(
            src_ref=src,
            dst_ref=dst,
            send_sem=send,
            recv_sem=recv,
            device_id=where,
            device_id_type=pl.DeviceIdType.MESH,
        )

    def obs_copy(i, peer, holder):
        return remote(obs_ref, obuf.at[holder], o_send.at[i], o_recv.at[i], member=peer)

    def t_copy(route, c, peer, holder):
        part = tbuf.at[holder, pl.ds(c * per, per)]
        return remote(part, part, t_send.at[route, c], t_recv.at[route, c], member=peer)

    vper = DEV_BLOCKS // V_CHUNKS

    def v_copy(route, c, peer, holder):
        part = vbuf.at[holder, pl.ds(c * vper, vper)]
        return remote(part, part, v_send.at[route, c], v_recv.at[route, c], member=peer)

    for i, peer in enumerate((near, far, cross)):
        obs_copy(i, peer, me).start()
    for c in range(T_CHUNKS):
        t_copy(1, c, far, me).start()
    for c in range(T_CHUNKS):
        t_copy(0, c, near, me).start()
    for c in range(V_CHUNKS):
        v_copy(1, c, far, me).start()
    for c in range(V_CHUNKS):
        v_copy(0, c, near, me).start()

    for i, holder in enumerate((near, far, cross)):
        obs_copy(i, holder, holder).wait_recv()

    rows = DEV_BLOCKS
    n_obs_rows = position.shape[0]
    values = jnp.concatenate([obuf[m, 0] for m in range(n_member)], axis=0)
    errors = jnp.concatenate([obuf[m, 1] for m in range(n_member)], axis=0)
    inverse = 1.0 / (errors * errors)
    parts = [*split3(inverse), *split3(values * inverse), *split3(values), jnp.ones_like(values)]
    slot_rows = lax.broadcasted_iota(jnp.int32, (rows, cb), 0)
    lane_rows = lax.broadcasted_iota(jnp.int32, (cb, cb), 0)
    acc = jnp.zeros((len(parts) * rows, cb), F32)
    for r in range(0, n_obs_rows, 2):
        left, right = [], []
        for q in (r, r + 1):
            hit = slot_rows == slot[q : q + 1]
            left.append(
                jnp.concatenate(
                    [jnp.where(hit, part[q : q + 1], 0.0) for part in parts], axis=0
                ).astype(BF16)
            )
            right.append(jnp.where(lane_rows == lane[q : q + 1], 1.0, 0.0).astype(BF16))
        acc = acc + dot_nt(jnp.concatenate(left, axis=1), jnp.concatenate(right, axis=1))
    tables = [acc[i * rows : (i + 1) * rows] for i in range(len(parts))]
    weight = tables[0] + tables[1] + tables[2]
    pull = tables[3] + tables[4] + tables[5]
    number = tables[9]
    centre = (tables[6] + tables[7] + tables[8]) / jnp.maximum(number, 1.0)
    scale = jnp.sqrt(weight)
    inverse_scale = jnp.where(weight > 0.0, 1.0 / jnp.maximum(scale, 1e-6), 0.0)
    wtab[0] = scale
    wtab[1] = pull * inverse_scale
    centre_parts = jnp.concatenate(split3(centre), axis=0).astype(BF16)
    apart = jnp.zeros((1, cb), F32)
    for q in range(n_obs_rows):
        onehot = jnp.where(lane_rows == lane[q : q + 1], 1.0, 0.0).astype(BF16)
        found = dot_nn(centre_parts, onehot)
        found = found[:rows] + found[rows : 2 * rows] + found[2 * rows :]
        found = jnp.sum(
            jnp.where(slot_rows == slot[q : q + 1], found, 0.0), axis=0, keepdims=True
        )
        apart = apart + (values[q : q + 1] - found) ** 2
    apart = jnp.sum(apart, axis=1, keepdims=True)
    error_sum = total(errors * errors)

    part_row = lax.broadcasted_iota(jnp.int32, (16, cb), 0)

    def forward(c):
        t_copy(1, c, far, far).wait_recv()
        t_copy(2, c, near, far).start()

    forward(0)

    def centre_chunk(c, carry):
        @pl.when(c + 1 < T_CHUNKS)
        def _():
            forward(c + 1)

        t_copy(0, c, near, near).wait_recv()
        t_copy(2, c, near, cross).wait_recv()
        for i in range(per):
            s = c * per + i
            x = jnp.concatenate([tbuf[m, s] for m in range(n_member)], axis=0).astype(F32)
            mean = jnp.sum(x, axis=0, keepdims=True) / K
            a = x - mean
            mtab[0, pl.ds(s, 1)] = mean
            mtab[1, pl.ds(s, 1)] = jnp.sum(a * a, axis=0, keepdims=True)
            row = wtab[0, pl.ds(s, 1)]
            hi, lo = split2(a * row)
            ubuf[s, :K] = hi
            ubuf[s, K : 2 * K] = lo
            v1, v2, v3 = split3(wtab[1, pl.ds(s, 1)] - mean * row)
            v = jnp.where(
                part_row == 0,
                v1,
                jnp.where(part_row == 1, v2, jnp.where(part_row == 2, v3, 0.0)),
            )
            ubuf[s, 2 * K :] = v.astype(BF16)
        return carry

    lax.fori_loop(0, T_CHUNKS, centre_chunk, 0)
    means = mtab[0]
    misfit = apart + total(number * (centre - means) ** 2)
    spread = error_sum + total(number * mtab[1]) / (K - 1)
    sum_rows = lax.broadcasted_iota(jnp.int32, (8, cb), 0)
    sums[pi] = jnp.where(sum_rows == 0, misfit, spread)

    def sum_copy(slot_index, peer):
        return remote(
            sums.at[slot_index],
            sums.at[slot_index],
            s_send.at[peer],
            s_recv.at[slot_index],
            patch=peer,
        )

    def send_sum(i, carry):
        sum_copy(pi, (pi + i) % n_patch).start()
        return carry

    lax.fori_loop(1, n_patch, send_sum, 0)

    def gram_of(p):
        acc = jnp.zeros((2 * K + 16, 2 * K), F32)
        for b in range(0, maxb, 2):
            pair = []
            for q in (b, b + 1):
                u = ubuf[jnp.minimum(start[p] + q, DEV_BLOCKS - 1)]
                pair.append(jnp.where(q < used[p], u, jnp.zeros_like(u)))
            pair = jnp.concatenate(pair, axis=1)
            acc = acc + dot_nt(pair, pair[: 2 * K])
        g = acc[:K] + acc[K : 2 * K]
        c = jnp.broadcast_to(jnp.sum(acc[2 * K :], axis=0, keepdims=True), (8, 2 * K))
        full = jnp.concatenate([g, c], axis=0)
        return full + pltpu.roll(full, K, 1)

    def edge_copy(i, peer):
        return remote(edge_send.at[i], edge_recv.at[i], e_send.at[i], e_recv.at[i], patch=peer)

    up = (pi + 1) % n_patch
    down = (pi + n_patch - 1) % n_patch
    gram = [None] * pd
    gram[pd - 1] = gram_of(pd - 1)
    edge_send[0] = gram[pd - 1]
    gram[0] = gram_of(0)
    edge_send[1] = gram[0]

    @pl.when(pi < n_patch - 1)
    def _():
        edge_copy(0, up).start()

    @pl.when(pi > 0)
    def _():
        edge_copy(1, down).start()

    for p in range(1, pd - 1):
        gram[p] = gram_of(p)
    for p in range(pd):
        grams[p] = gram[p]

    def relay(c, carry):
        v_copy(1, c, far, far).wait_recv()
        v_copy(2, c, near, far).start()
        return carry

    lax.fori_loop(0, V_CHUNKS, relay, 0)

    @pl.when(pi > 0)
    def _():
        edge_copy(0, up).wait_recv()

    @pl.when(pi == 0)
    def _():
        edge_recv[0] = jnp.zeros(edge_recv.shape[1:], F32)

    @pl.when(pi < n_patch - 1)
    def _():
        edge_copy(1, down).wait_recv()

    @pl.when(pi == n_patch - 1)
    def _():
        edge_recv[1] = jnp.zeros(edge_recv.shape[1:], F32)

    def recv_sum(i, carry):
        peer = (pi + i) % n_patch
        sum_copy(peer, peer).wait_recv()
        return carry

    lax.fori_loop(1, n_patch, recv_sum, 0)
    both = jnp.sum(sums[...], axis=0)
    inflation = both[0:1] / both[1:2]
    inflation_ref[0, 0] = jnp.max(inflation)

    eye = jnp.where(
        lax.broadcasted_iota(jnp.int32, (K, K), 0) == lax.broadcasted_iota(jnp.int32, (K, K), 1),
        1.0,
        0.0,
    )
    field = [edge_recv[0]] + [grams[p] for p in range(pd)] + [edge_recv[1]]
    ridge = (K - 1) / inflation[:, :K]
    square, norm, drive = [], [], []
    for p in range(pd):
        local_field = field[p + 1] + neighbour_weight * (field[p] + field[p + 2])
        system = local_field[:K, :K] + ridge * eye
        drive.append(local_field[K : K + 1, :K])
        size = jnp.sqrt(total(system * system))
        norm.append(size)
        square.append(system / size)
    middle = [1.5 * eye - 0.5 * a for a in square]
    inverse_part = middle
    m_parts = [split2(a) for a in middle]
    z_parts = m_parts
    s_parts = [split2(a) for a in square]
    for sweep in range(1, NS_STEPS):
        square = [product(a, b) for a, b in zip(s_parts, m_parts)]
        s_parts = [split2(a) for a in square]
        middle = [1.5 * eye - 0.5 * product(a, b) for a, b in zip(z_parts, s_parts)]
        m_parts = [split2(a) for a in middle]
        inverse_part = [product(a, b) for a, b in zip(m_parts, z_parts)]
        z_parts = [split2(a) for a in inverse_part]
    for p in range(pd):
        root = inverse_part[p] / jnp.sqrt(norm[p])
        inner = jnp.sum(root * drive[p], axis=1, keepdims=True)
        mean_weights = jnp.sum(root * inner, axis=0, keepdims=True)
        roots[p] = mean_weights + math.sqrt(K - 1) * root
        mine = roots[p, pl.ds(me * local, local)].astype(BF16)
        weights[p, :local] = mine
        weights[p, local:] = jnp.ones((16, K), BF16)
        short = (1.0 - jnp.sum(mine.astype(F32), axis=1, keepdims=True)) / K
        defect[p] = jnp.broadcast_to(short, (local, cb))

    def finish_chunk(c, carry):
        v_copy(0, c, near, near).wait_recv()
        v_copy(2, c, near, cross).wait_recv()
        for i in range(vper):
            s = c * vper + i
            p, _ = patch_of(s)
            w = weights[p]
            d = defect[p]
            thick = jnp.concatenate([tbuf[m, s] for m in range(n_member)], axis=0)
            speeds = [
                jnp.concatenate([vbuf[m, s, v] for m in range(n_member)], axis=0)
                for v in range(nv - 1)
            ]
            got = dot_nn(w, jnp.concatenate([thick] + speeds, axis=1))
            for v in range(nv):
                g = got[:, v * cb : (v + 1) * cb]
                res[s, v] = (g[:local] + g[local : local + 1] * d).astype(BF16)
        return carry

    lax.fori_loop(0, V_CHUNKS, finish_chunk, 0)

    for i, peer in enumerate((near, far, cross)):
        obs_copy(i, peer, me).wait_send()
    for c in range(T_CHUNKS):
        t_copy(0, c, near, me).wait_send()
        t_copy(1, c, far, me).wait_send()
        t_copy(2, c, near, far).wait_send()
    for c in range(V_CHUNKS):
        v_copy(0, c, near, me).wait_send()
        v_copy(1, c, far, me).wait_send()
        v_copy(2, c, near, far).wait_send()

    @pl.when(pi < n_patch - 1)
    def _():
        edge_copy(0, up).wait_send()

    @pl.when(pi > 0)
    def _():
        edge_copy(1, down).wait_send()

    def sum_left(i, carry):
        sum_copy(pi, (pi + i) % n_patch).wait_send()
        return carry

    lax.fori_loop(1, n_patch, sum_left, 0)


def expand_kernel(pd, used_ref, inflation_in, res, out_ref, inflation_out):
    p = pl.program_id(0)
    first = lax.axis_index("patch") * pd
    start = jnp.int32(0)
    for q in range(pd):
        start = start + jnp.where(q < p, used_ref[first + q], 0)
    used = used_ref[first + p]
    for b in range(out_ref.shape[1]):
        r = res[jnp.minimum(start + b, DEV_BLOCKS - 1)]
        out_ref[0, b] = jnp.where(b < used, r, jnp.zeros_like(r))
    inflation_out[0, 0] = inflation_in[0, 0]


def solution(mesh):
    n_patch, n_member = mesh.shape["patch"], mesh.shape["member"]

    def per_device(background, patch_blocks, obs_values, obs_errors, obs_patch, obs_position):
        pd, maxb, nv, local, cb = background.shape
        values, errors = obs_values.reshape(-1, cb), obs_errors.reshape(-1, cb)
        slot_patch, position = obs_patch.reshape(-1, cb), obs_position.reshape(-1, cb)
        vmem = pl.BlockSpec(memory_space=pltpu.VMEM)
        smem = pl.BlockSpec(memory_space=pltpu.SMEM)
        hbm = pl.BlockSpec(memory_space=pl.ANY)
        dma = pltpu.SemaphoreType.DMA
        packed, ratio = pl.pallas_call(
            functools.partial(kernel, n_patch, n_member),
            out_shape=(
                jax.ShapeDtypeStruct((DEV_BLOCKS, nv, local, cb), BF16),
                jax.ShapeDtypeStruct((1, 1), F32),
            ),
            in_specs=[
                smem,
                hbm,
                hbm,
                hbm,
                hbm,
                hbm,
            ],
            out_specs=(vmem, smem),
            scratch_shapes=[
                pltpu.VMEM(background.shape, BF16),
                pltpu.VMEM((2, *values.shape), F32),
                pltpu.VMEM(slot_patch.shape, jnp.int32),
                pltpu.VMEM(position.shape, jnp.int32),
                pltpu.VMEM((n_member, DEV_BLOCKS, local, cb), BF16),
                pltpu.VMEM((n_member, DEV_BLOCKS, nv - 1, local, cb), BF16),
                pltpu.VMEM((n_member, 2, *values.shape), F32),
                pltpu.VMEM((2, DEV_BLOCKS, cb), F32),
                pltpu.VMEM((2, DEV_BLOCKS, cb), F32),
                pltpu.VMEM((DEV_BLOCKS, 2 * K + 16, cb), BF16),
                pltpu.VMEM((2, K + 8, 2 * K), F32),
                pltpu.VMEM((2, K + 8, 2 * K), F32),
                pltpu.VMEM((n_patch, 8, cb), F32),
                pltpu.VMEM((pd, K + 8, 2 * K), F32),
                pltpu.VMEM((pd, K, K), F32),
                pltpu.VMEM((pd, local + 16, K), BF16),
                pltpu.VMEM((pd, local, cb), F32),
                dma,
                dma((4,)),
                dma((3, T_CHUNKS)),
                dma((3, T_CHUNKS)),
                dma((3, V_CHUNKS)),
                dma((3, V_CHUNKS)),
                dma((3,)),
                dma((3,)),
                dma((2,)),
                dma((2,)),
                dma((n_patch,)),
                dma((n_patch,)),
            ],
            compiler_params=pltpu.CompilerParams(collective_id=0, has_side_effects=True),
        )(
            patch_blocks,
            values,
            errors,
            slot_patch,
            position,
            background,
        )
        analysis, inflation = pl.pallas_call(
            functools.partial(expand_kernel, pd),
            grid=(pd,),
            out_shape=(
                jax.ShapeDtypeStruct(background.shape, BF16),
                jax.ShapeDtypeStruct((1, 1), F32),
            ),
            in_specs=[smem, smem, vmem],
            out_specs=(
                pl.BlockSpec((1, maxb, nv, local, cb), lambda p: (p, 0, 0, 0, 0)),
                smem,
            ),
        )(patch_blocks, ratio, packed)
        return analysis, inflation.reshape(())

    in_specs = (
        P("patch", None, None, "member", None),
        P(),
        P(("patch", "member")),
        P(("patch", "member")),
        P("patch"),
        P("patch"),
    )
    out_specs = (P("patch", None, None, "member", None), P())
    return jax.shard_map(
        per_device, mesh=mesh, in_specs=in_specs, out_specs=out_specs, check_vma=False
    )
```
